32 devices in a mesh: groups: 2 (over y), store: 8 (over z, x), tensor: 2 (over core).
Axes of the slice: x: 2, y: 2, z: 4, core: 2. Of those that a mesh axis runs over, the one named last changes fastest.
Arguments:
- queries: bfloat16 [32, 8192], P(('groups', 'store'), 'tensor'), parts along dimension 0, may hold values from -200 to 200
- new_kv: bfloat16 [32, 2, 1024], P(('groups', 'store'), None, 'tensor'), parts along dimension 0, may hold values from -15 to 15
- kv_pages: bfloat16 [128, 2, 256, 1024], P(('groups', 'store'), None, None, 'tensor'), parts along dimension 0, may hold values from -15 to 15
- page_index: int32 [32, 4], P(('groups', 'store')), parts along dimension 0, may hold values from 0 to 7
- page_owner: int32 [32, 4], P(('groups', 'store')), parts along dimension 0, may hold values from 0 to 7, as said below
- seq_pages: int32 [32], P(('groups', 'store')), parts along dimension 0, may hold values from 1 to 4, as said below
Outputs:
- attended: bfloat16 [32, 8192], P(('groups', 'store'), 'tensor'), parts along dimension 0
The draws below stay inside these ranges and needn't reach their ends.
There are 2 independent parts, one for each index of `groups`. The reference program is written for one: setup_inputs(seed, part) draws one part's arguments, and reference() takes and returns one part's arrays. A program takes and returns all parts, laid end to end along the dimension named above; each array names one. Nothing has to cross between parts.
Inputs may be any that keep to these rules, and one draw needn't show every extreme that they name: `page_owner`: page j of sequence s lies on store index (s // 2 + o) modulo the number of store indices, with o from 0 to 3; over the slots of the sequences of one store index, at most 2 share one o, so at most 2 live pages of those sequences lie on one store index. `seq_pages`: the sequences of store index 0 all have 4 pages.
All inputs are finite; a program needn't handle non-finite values.
Results may differ from the reference program's by a relative error of at most 0.0011.
Values may be sent and summed in bfloat16 or wider, within the bound.
A program may use at most 64 MiB of HBM per device.

```python
import jax
import jax.numpy as jnp
from jax import lax

HEADS = 64
KV_HEADS = 8
HEAD_DIM = 128
PAGE = 256
MAXP = 4
B_DEV = 2
GROUP = 8
CAP = 2
P_DEV = 8
SEQS = 16
PAGES = 64


def draw_queries(key, part):
    first = jax.random.fold_in(key, 0)
    base = jax.random.normal(first, (SEQS, HEADS * HEAD_DIM), jnp.float32)
    return jnp.clip(base, -200.0, 200.0).astype(jnp.bfloat16)


def draw_page_owner(key, part):
    shards = SEQS // B_DEV
    entries = B_DEV * MAXP
    keys = jax.random.split(jax.random.fold_in(key, 11), shards)
    orders = jax.vmap(lambda single: jax.random.permutation(single, entries))(keys)
    page_starts = orders // CAP
    shard_holders = (jnp.arange(shards, dtype=jnp.int32)[:, None] + page_starts) % shards
    return shard_holders.reshape(SEQS, MAXP).astype(jnp.int32)


def draw_seq_pages(key, part):
    counts = jax.random.randint(jax.random.fold_in(key, 23), (SEQS,), 1, MAXP + 1, dtype=jnp.int32)
    return counts.at[:B_DEV].set(MAXP)


def plant(drawn, key, low, high):
    index_at = [jax.random.randint(jax.random.fold_in(key, axis), (), 0, length) for axis, length in enumerate(drawn.shape)]
    widest = drawn.shape.index(max(drawn.shape))
    next_to = index_at[:widest] + [(index_at[widest] + 1) % drawn.shape[widest]] + index_at[widest + 1:]
    return drawn.at[tuple(index_at)].set(low).at[tuple(next_to)].set(high)


def level_of(key, dims, cuts, smallest, top_value):
    def one(axis_at, blocks):
        steps = jax.random.uniform(jax.random.fold_in(jax.random.fold_in(key, 6), axis_at), (blocks,), jnp.float32, smallest / len(cuts), top_value / len(cuts))
        return jnp.repeat(jnp.exp(steps), dims[axis_at] // blocks).reshape((-1,) + (1,) * (len(dims) - axis_at - 1))

    level = one(*cuts[0])
    for cut in cuts[1:]:
        level = level * one(*cut)
    return level


def centred(key, shape, scale, reach, cuts=(), kind=jnp.bfloat16):
    array = jax.random.normal(key, shape, jnp.float32) * scale
    if len(cuts) > 0:
        array = level_of(key, shape, cuts, -0.22, 0.18) * array
    return jnp.clip(array, min=-reach, max=reach).astype(kind)


def setup_inputs(seed: int = 0, part: int = 0) -> dict:
    splits = jax.random.split(jax.random.key(seed), 7)
    part_splits = jax.random.split(jax.random.fold_in(splits[6], part), 7)
    queries = draw_queries(jax.random.fold_in(jax.random.fold_in(splits[6], part), 71), part)
    new_kv = centred(part_splits[1], (SEQS, 2, KV_HEADS * HEAD_DIM), 2.5, 15.0, ((0, 8), (2, 2)))
    kv_pages = centred(part_splits[2], (PAGES, 2, PAGE, KV_HEADS * HEAD_DIM), 2.5, 15.0, ((0, 8), (3, 2)))
    page_index = plant(jax.random.randint(part_splits[3], (SEQS, MAXP), 0, P_DEV), jax.random.fold_in(part_splits[3], 1), 0, P_DEV - 1).astype(jnp.int32)
    page_owner = draw_page_owner(jax.random.fold_in(jax.random.fold_in(splits[6], part), 71), part)
    seq_pages = draw_seq_pages(jax.random.fold_in(jax.random.fold_in(splits[6], part), 71), part)
    return {"queries": queries, "new_kv": new_kv, "kv_pages": kv_pages, "page_index": page_index, "page_owner": page_owner, "seq_pages": seq_pages}


def reference(queries, new_kv, kv_pages, page_index, page_owner, seq_pages):
    scale = HEAD_DIM ** -0.5

    def single_request_attend(items):
        query, fresh, places, shard_holders, length = items
        rows = (shard_holders * P_DEV + places).astype(jnp.int32)
        chosen = kv_pages[rows]
        keys = chosen[:, 0].reshape(MAXP * PAGE, KV_HEADS, HEAD_DIM).astype(jnp.float32)
        values = chosen[:, 1].reshape(MAXP * PAGE, KV_HEADS, HEAD_DIM).astype(jnp.float32)
        live = (jnp.arange(MAXP * PAGE, dtype=jnp.int32) // PAGE) < length
        heads = query.reshape(KV_HEADS, GROUP, HEAD_DIM).astype(jnp.float32)
        new_key = fresh[0].reshape(KV_HEADS, HEAD_DIM).astype(jnp.float32)
        new_value = fresh[1].reshape(KV_HEADS, HEAD_DIM).astype(jnp.float32)
        scores = jnp.einsum("kgd,pkd->kgp", heads, keys, precision=lax.Precision.HIGHEST) * scale
        own = jnp.einsum("kgd,kd->kg", heads, new_key, precision=lax.Precision.HIGHEST) * scale
        masked = jnp.where(live[None, None, :], scores, jnp.float32(-1e30))
        peak = jnp.maximum(jnp.max(masked, axis=-1), own)
        weights = jnp.where(live[None, None, :], jnp.exp(masked - peak[..., None]), jnp.float32(0.0))
        own_weight = jnp.exp(own - peak)
        total = jnp.sum(weights, axis=-1) + own_weight
        summed = jnp.einsum("kgp,pkd->kgd", weights, values, precision=lax.Precision.HIGHEST)
        summed = summed + own_weight[..., None] * new_value[:, None, :]
        return (summed / total[..., None]).reshape(-1).astype(jnp.bfloat16)

    return lax.map(single_request_attend, (queries, new_kv, page_index, page_owner, seq_pages))
```

```python
import functools

import jax
import jax.numpy as jnp
from jax import lax
from jax.experimental import pallas as pl
from jax.experimental.pallas import tpu as pltpu
from jax.sharding import PartitionSpec as P

HEAD_DIM = 128
REACH = 4
MASKED = -1e30
FLOOR = -1e29
MESH = pl.DeviceIdType.MESH


def plan(places, owners, lengths, slot, me, seq_count, most_pages, capacity):
    pages = [jnp.int32(0)] * capacity
    seqs = [jnp.int32(-1)] * capacity
    rank = jnp.int32(0)
    for s in range(seq_count):
        length = lengths[slot, 0, s]
        for j in range(most_pages):
            hit = jnp.logical_and(j < length, owners[slot, s, j] == me)
            place = places[slot, s, j]
            for c in range(capacity):
                mine = jnp.logical_and(hit, rank == c)
                pages[c] = jnp.where(mine, place, pages[c])
                seqs[c] = jnp.where(mine, s, seqs[c])
            rank = rank + hit.astype(jnp.int32)
    return pages, seqs


def kernel(
    n, seq_count, most_pages, capacity, kv_count, rows, order, scale,
    q_ref, fresh_ref, kv_ref, places_ref, owners_ref, lengths_ref, out_ref,
    key_shelf, value_shelf, q_in, fresh, places, owners, lengths, part_out, part_in,
    shelf_sem, local_sem, ask_send, ask_recv, back_send, back_recv,
):
    me = lax.axis_index("store")

    def at(steps):
        return {"store": lax.rem(me + steps + n, n)}

    loads = [
        pltpu.make_async_copy(kv_ref.at[:, i], half, shelf_sem.at[i])
        for i, half in enumerate((key_shelf, value_shelf))
    ]
    asked = ((q_ref, q_in), (places_ref, places), (owners_ref, owners), (lengths_ref, lengths))
    locals_ = [
        pltpu.make_async_copy(source, target.at[0], local_sem.at[i])
        for i, (source, target) in enumerate(asked)
    ]
    locals_.append(pltpu.make_async_copy(fresh_ref, fresh, local_sem.at[len(asked)]))

    barrier = pltpu.get_barrier_semaphore()
    for d in range(1, REACH):
        for sign in (1, -1):
            pl.semaphore_signal(barrier, inc=1, device_id=at(sign * d), device_id_type=MESH)
    for copy in locals_ + loads:
        copy.start()
    pl.semaphore_wait(barrier, 2 * (REACH - 1))

    asks = {}
    for d in reversed(order):
        asks[d] = [
            pltpu.make_async_remote_copy(
                src_ref=source,
                dst_ref=target.at[d],
                send_sem=ask_send.at[i, d - 1],
                recv_sem=ask_recv.at[i, d - 1],
                device_id=at(d),
                device_id_type=MESH,
            )
            for i, (source, target) in enumerate(asked)
        ]
        for copy in asks[d]:
            copy.start()

    turn = lax.rem(lax.broadcasted_iota(jnp.int32, (rows, 1), 0), seq_count)
    lane = lax.broadcasted_iota(jnp.int32, (rows, HEAD_DIM), 1)

    def partial_of(slot, wait_values=None):
        pages, seqs = plan(places, owners, lengths, slot, me, seq_count, most_pages, capacity)
        bias = [jnp.where(turn == seq, jnp.float32(0.0), jnp.float32(MASKED)) for seq in seqs]
        scores = []
        for k in range(kv_count):
            qk = q_in[slot, k * rows : (k + 1) * rows, :]
            row = []
            for c in range(capacity):
                keys = key_shelf[pages[c], :, k * HEAD_DIM : (k + 1) * HEAD_DIM]
                dots = lax.dot_general(
                    qk, keys, (((1,), (1,)), ((), ())), preferred_element_type=jnp.float32
                )
                row.append(dots * scale + bias[c])
            scores.append(row)
        if wait_values is not None:
            wait_values()
        peaks, totals, sums = [], [], []
        for k in range(kv_count):
            peak = functools.reduce(jnp.maximum, [jnp.max(s, axis=1, keepdims=True) for s in scores[k]])
            peak = jnp.maximum(peak, jnp.float32(FLOOR))
            total = jnp.float32(0.0)
            summed = jnp.float32(0.0)
            for c in range(capacity):
                w = jnp.exp(scores[k][c] - peak)
                total = total + jnp.sum(w, axis=1, keepdims=True)
                high = w.astype(jnp.bfloat16)
                low = (w - high.astype(jnp.float32)).astype(jnp.bfloat16)
                values = value_shelf[pages[c], :, k * HEAD_DIM : (k + 1) * HEAD_DIM]
                summed = summed + jnp.dot(
                    jnp.concatenate([high, low], axis=0), values, preferred_element_type=jnp.float32
                )
            peaks.append(peak)
            totals.append(total)
            sums.append(summed[:rows] + summed[rows:])
        return peaks, totals, sums

    for copy in locals_:
        copy.wait()
    loads[0].wait()
    peaks, totals, sums = partial_of(0, loads[1].wait)
    for k in range(kv_count):
        qk = q_in[0, k * rows : (k + 1) * rows, :].astype(jnp.float32)
        cut = slice(k * HEAD_DIM, (k + 1) * HEAD_DIM)
        key = fresh[0, 0:1, cut].astype(jnp.float32)
        value = fresh[0, 1:2, cut].astype(jnp.float32)
        for s in range(1, seq_count):
            key = jnp.where(turn == s, fresh[s, 0:1, cut].astype(jnp.float32), key)
            value = jnp.where(turn == s, fresh[s, 1:2, cut].astype(jnp.float32), value)
        own = jnp.sum(qk * key, axis=1, keepdims=True) * scale
        peak = jnp.maximum(peaks[k], own)
        factor = jnp.exp(peaks[k] - peak)
        weight = jnp.exp(own - peak)
        peaks[k] = peak
        totals[k] = totals[k] * factor + weight
        sums[k] = sums[k] * factor + weight * value

    backs = {}
    for d in order:
        for copy in asks[d]:
            copy.wait_recv()
        theirs = partial_of(d)
        stats = jnp.zeros((rows, HEAD_DIM), jnp.float32)
        for k in range(kv_count):
            part_out[d - 1, k * rows : (k + 1) * rows, :] = theirs[2][k]
            stats = jnp.where(lane == 2 * k, theirs[0][k], stats)
            stats = jnp.where(lane == 2 * k + 1, theirs[1][k], stats)
        part_out[d - 1, kv_count * rows :, :] = stats
        backs[d] = pltpu.make_async_remote_copy(
            src_ref=part_out.at[d - 1],
            dst_ref=part_in.at[d - 1],
            send_sem=back_send.at[d - 1],
            recv_sem=back_recv.at[d - 1],
            device_id=at(-d),
            device_id_type=MESH,
        )
        backs[d].start()

    for d in order:
        backs[d].wait_recv()
    for k in range(kv_count):
        part_peaks = [part_in[d - 1, kv_count * rows :, 2 * k : 2 * k + 1] for d in order]
        part_totals = [part_in[d - 1, kv_count * rows :, 2 * k + 1 : 2 * k + 2] for d in order]
        highest = functools.reduce(jnp.maximum, part_peaks, peaks[k])
        factor = jnp.exp(peaks[k] - highest)
        total = totals[k] * factor
        summed = sums[k] * factor
        for i, d in enumerate(order):
            factor = jnp.exp(part_peaks[i] - highest)
            total = total + part_totals[i] * factor
            summed = summed + part_in[d - 1, k * rows : (k + 1) * rows, :] * factor
        out_ref[k * rows : (k + 1) * rows, :] = (summed / total).astype(out_ref.dtype)
    for d in order:
        for copy in asks[d]:
            copy.wait_send()
        backs[d].wait_send()


def body(queries, new_kv, kv_pages, page_index, page_owner, seq_pages):
    n = lax.axis_size("store")
    seq_count, most_pages = page_index.shape
    kv_count = new_kv.shape[2] // HEAD_DIM
    heads = queries.shape[1] // HEAD_DIM
    rows = heads // kv_count * seq_count
    all_rows = heads * seq_count
    capacity = seq_count * most_pages // REACH
    q = queries.reshape(seq_count, heads, HEAD_DIM).transpose(1, 0, 2).reshape(all_rows, HEAD_DIM)
    away = REACH - 1
    half = kv_pages.shape[:1] + kv_pages.shape[2:]
    order = (2, 1) + tuple(range(3, REACH))
    out = pl.pallas_call(
        functools.partial(
            kernel, n, seq_count, most_pages, capacity, kv_count, rows, order, HEAD_DIM ** (-0.5)
        ),
        out_shape=jax.ShapeDtypeStruct((all_rows, HEAD_DIM), jnp.bfloat16),
        in_specs=[pl.BlockSpec(memory_space=pl.ANY)] * 6,
        out_specs=pl.BlockSpec(memory_space=pltpu.VMEM),
        scratch_shapes=[
            pltpu.VMEM(half, kv_pages.dtype),
            pltpu.VMEM(half, kv_pages.dtype),
            pltpu.VMEM((REACH, all_rows, HEAD_DIM), q.dtype),
            pltpu.VMEM(new_kv.shape, new_kv.dtype),
            pltpu.SMEM((REACH, seq_count, most_pages), jnp.int32),
            pltpu.SMEM((REACH, seq_count, most_pages), jnp.int32),
            pltpu.SMEM((REACH, 1, seq_count), jnp.int32),
            pltpu.VMEM((away, all_rows + rows, HEAD_DIM), jnp.float32),
            pltpu.VMEM((away, all_rows + rows, HEAD_DIM), jnp.float32),
            pltpu.SemaphoreType.DMA((2,)),
            pltpu.SemaphoreType.DMA((5,)),
            pltpu.SemaphoreType.DMA((4, away)),
            pltpu.SemaphoreType.DMA((4, away)),
            pltpu.SemaphoreType.DMA((away,)),
            pltpu.SemaphoreType.DMA((away,)),
        ],
        compiler_params=pltpu.CompilerParams(collective_id=0, has_side_effects=True),
    )(q, new_kv, kv_pages, page_index, page_owner, seq_pages.reshape(1, seq_count))
    out = out.reshape(heads, seq_count, HEAD_DIM).transpose(1, 0, 2)
    return out.reshape(seq_count, heads * HEAD_DIM)


def solution(mesh):
    in_specs = (
        P(("groups", "store"), "tensor"),
        P(("groups", "store"), None, "tensor"),
        P(("groups", "store"), None, None, "tensor"),
        P(("groups", "store"), None),
        P(("groups", "store"), None),
        P(("groups", "store")),
    )
    out_specs = P(("groups", "store"), "tensor")
    return jax.shard_map(body, mesh=mesh, in_specs=in_specs, out_specs=out_specs, check_vma=False)
```

```python
import functools

import jax
import jax.numpy as jnp
from jax import lax
from jax.experimental import pallas as pl
from jax.experimental.pallas import tpu as pltpu
from jax.sharding import PartitionSpec as P

HEAD_DIM = 128
REACH = 4
MASKED = -1e30
FLOOR = -1e29
MESH = pl.DeviceIdType.MESH


def plan(places, owners, lengths, slot, me, seq_count, most_pages, capacity):
    pages = [jnp.int32(0)] * capacity
    seqs = [jnp.int32(-1)] * capacity
    rank = jnp.int32(0)
    for s in range(seq_count):
        length = lengths[slot, 0, s]
        for j in range(most_pages):
            hit = jnp.logical_and(j < length, owners[slot, s, j] == me)
            place = places[slot, s, j]
            for c in range(capacity):
                mine = jnp.logical_and(hit, rank == c)
                pages[c] = jnp.where(mine, place, pages[c])
                seqs[c] = jnp.where(mine, s, seqs[c])
            rank = rank + hit.astype(jnp.int32)
    return pages, seqs


def kernel(
    n, seq_count, most_pages, capacity, kv_count, rows, order, scale,
    q_ref, fresh_ref, kv_ref, places_ref, owners_ref, lengths_ref, out_ref,
    key_shelf, value_shelf, q_in, fresh, places, owners, lengths, part_out, part_in,
    shelf_sem, local_sem, ask_send, ask_recv, back_send, back_recv,
):
    me = lax.axis_index("store")

    def at(steps):
        return {"store": lax.rem(me + steps + n, n)}

    loads = [
        pltpu.make_async_copy(kv_ref.at[:, i], half, shelf_sem.at[i])
        for i, half in enumerate((key_shelf, value_shelf))
    ]
    asked = ((q_ref, q_in), (places_ref, places), (owners_ref, owners), (lengths_ref, lengths))
    locals_ = [
        pltpu.make_async_copy(source, target.at[0], local_sem.at[i])
        for i, (source, target) in enumerate(asked)
    ]
    locals_.append(pltpu.make_async_copy(fresh_ref, fresh, local_sem.at[len(asked)]))

    barrier = pltpu.get_barrier_semaphore()
    for d in range(1, REACH):
        for sign in (1, -1):
            pl.semaphore_signal(barrier, inc=1, device_id=at(sign * d), device_id_type=MESH)
    for copy in locals_ + loads:
        copy.start()
    for copy in locals_:
        copy.wait()
    pl.semaphore_wait(barrier, 2 * (REACH - 1))

    asks = {}
    for d in reversed(order):
        asks[d] = [
            pltpu.make_async_remote_copy(
                src_ref=target.at[0],
                dst_ref=target.at[d],
                send_sem=ask_send.at[i, d - 1],
                recv_sem=ask_recv.at[i, d - 1],
                device_id=at(d),
                device_id_type=MESH,
            )
            for i, (source, target) in enumerate(asked)
        ]
        for copy in asks[d]:
            copy.start()

    turn = lax.rem(lax.broadcasted_iota(jnp.int32, (rows, 1), 0), seq_count)
    lane = lax.broadcasted_iota(jnp.int32, (rows, HEAD_DIM), 1)

    def partial_of(slot, wait_values=None):
        pages, seqs = plan(places, owners, lengths, slot, me, seq_count, most_pages, capacity)
        bias = [jnp.where(turn == seq, jnp.float32(0.0), jnp.float32(MASKED)) for seq in seqs]
        scores = []
        for k in range(kv_count):
            qk = q_in[slot, k * rows : (k + 1) * rows, :]
            row = []
            for c in range(capacity):
                keys = key_shelf[pages[c], :, k * HEAD_DIM : (k + 1) * HEAD_DIM]
                dots = lax.dot_general(
                    qk, keys, (((1,), (1,)), ((), ())), preferred_element_type=jnp.float32
                )
                row.append(dots * scale + bias[c])
            scores.append(row)
        if wait_values is not None:
            wait_values()
        peaks, totals, sums = [], [], []
        for k in range(kv_count):
            peak = functools.reduce(jnp.maximum, [jnp.max(s, axis=1, keepdims=True) for s in scores[k]])
            peak = jnp.maximum(peak, jnp.float32(FLOOR))
            total = jnp.float32(0.0)
            summed = jnp.float32(0.0)
            for c in range(capacity):
                w = jnp.exp(scores[k][c] - peak)
                total = total + jnp.sum(w, axis=1, keepdims=True)
                high = w.astype(jnp.bfloat16)
                low = (w - high.astype(jnp.float32)).astype(jnp.bfloat16)
                values = value_shelf[pages[c], :, k * HEAD_DIM : (k + 1) * HEAD_DIM]
                summed = summed + jnp.dot(
                    jnp.concatenate([high, low], axis=0), values, preferred_element_type=jnp.float32
                )
            peaks.append(peak)
            totals.append(total)
            sums.append(summed[:rows] + summed[rows:])
        return peaks, totals, sums

    loads[0].wait()
    peaks, totals, sums = partial_of(0, loads[1].wait)
    for k in range(kv_count):
        qk = q_in[0, k * rows : (k + 1) * rows, :].astype(jnp.float32)
        cut = slice(k * HEAD_DIM, (k + 1) * HEAD_DIM)
        key = fresh[0, 0:1, cut].astype(jnp.float32)
        value = fresh[0, 1:2, cut].astype(jnp.float32)
        for s in range(1, seq_count):
            key = jnp.where(turn == s, fresh[s, 0:1, cut].astype(jnp.float32), key)
            value = jnp.where(turn == s, fresh[s, 1:2, cut].astype(jnp.float32), value)
        own = jnp.sum(qk * key, axis=1, keepdims=True) * scale
        peak = jnp.maximum(peaks[k], own)
        factor = jnp.exp(peaks[k] - peak)
        weight = jnp.exp(own - peak)
        peaks[k] = peak
        totals[k] = totals[k] * factor + weight
        sums[k] = sums[k] * factor + weight * value

    backs = {}
    for d in order:
        for copy in asks[d]:
            copy.wait_recv()
        theirs = partial_of(d)
        stats = jnp.zeros((rows, HEAD_DIM), jnp.float32)
        for k in range(kv_count):
            part_out[d - 1, k * rows : (k + 1) * rows, :] = theirs[2][k]
            stats = jnp.where(lane == 2 * k, theirs[0][k], stats)
            stats = jnp.where(lane == 2 * k + 1, theirs[1][k], stats)
        part_out[d - 1, kv_count * rows :, :] = stats
        backs[d] = pltpu.make_async_remote_copy(
            src_ref=part_out.at[d - 1],
            dst_ref=part_in.at[d - 1],
            send_sem=back_send.at[d - 1],
            recv_sem=back_recv.at[d - 1],
            device_id=at(-d),
            device_id_type=MESH,
        )
        backs[d].start()

    for d in order:
        backs[d].wait_recv()
    for k in range(kv_count):
        part_peaks = [part_in[d - 1, kv_count * rows :, 2 * k : 2 * k + 1] for d in order]
        part_totals = [part_in[d - 1, kv_count * rows :, 2 * k + 1 : 2 * k + 2] for d in order]
        highest = functools.reduce(jnp.maximum, part_peaks, peaks[k])
        factor = jnp.exp(peaks[k] - highest)
        total = totals[k] * factor
        summed = sums[k] * factor
        for i, d in enumerate(order):
            factor = jnp.exp(part_peaks[i] - highest)
            total = total + part_totals[i] * factor
            summed = summed + part_in[d - 1, k * rows : (k + 1) * rows, :] * factor
        out_ref[k * rows : (k + 1) * rows, :] = (summed / total).astype(out_ref.dtype)
    for d in order:
        for copy in asks[d]:
            copy.wait_send()
        backs[d].wait_send()


def body(queries, new_kv, kv_pages, page_index, page_owner, seq_pages):
    n = lax.axis_size("store")
    seq_count, most_pages = page_index.shape
    kv_count = new_kv.shape[2] // HEAD_DIM
    heads = queries.shape[1] // HEAD_DIM
    rows = heads // kv_count * seq_count
    all_rows = heads * seq_count
    capacity = seq_count * most_pages // REACH
    q = queries.reshape(seq_count, heads, HEAD_DIM).transpose(1, 0, 2).reshape(all_rows, HEAD_DIM)
    away = REACH - 1
    half = kv_pages.shape[:1] + kv_pages.shape[2:]
    order = (1, 2, 3)
    out = pl.pallas_call(
        functools.partial(
            kernel, n, seq_count, most_pages, capacity, kv_count, rows, order, HEAD_DIM ** (-0.5)
        ),
        out_shape=pltpu.VMEM((all_rows, HEAD_DIM), jnp.bfloat16),
        in_specs=[pl.BlockSpec(memory_space=pl.ANY)] * 6,
        out_specs=pl.BlockSpec(memory_space=pltpu.VMEM),
        scratch_shapes=[
            pltpu.VMEM(half, kv_pages.dtype),
            pltpu.VMEM(half, kv_pages.dtype),
            pltpu.VMEM((REACH, all_rows, HEAD_DIM), q.dtype),
            pltpu.VMEM(new_kv.shape, new_kv.dtype),
            pltpu.SMEM((REACH, seq_count, most_pages), jnp.int32),
            pltpu.SMEM((REACH, seq_count, most_pages), jnp.int32),
            pltpu.SMEM((REACH, 1, seq_count), jnp.int32),
            pltpu.VMEM((away, all_rows + rows, HEAD_DIM), jnp.float32),
            pltpu.VMEM((away, all_rows + rows, HEAD_DIM), jnp.float32),
            pltpu.SemaphoreType.DMA((2,)),
            pltpu.SemaphoreType.DMA((5,)),
            pltpu.SemaphoreType.DMA((4, away)),
            pltpu.SemaphoreType.DMA((4, away)),
            pltpu.SemaphoreType.DMA((away,)),
            pltpu.SemaphoreType.DMA((away,)),
        ],
        compiler_params=pltpu.CompilerParams(collective_id=0, has_side_effects=True),
    )(q, new_kv, kv_pages, page_index, page_owner, seq_pages.reshape(1, seq_count))
    out = out.reshape(heads, seq_count, HEAD_DIM).transpose(1, 0, 2)
    return out.reshape(seq_count, heads * HEAD_DIM)


def solution(mesh):
    in_specs = (
        P(("groups", "store"), "tensor"),
        P(("groups", "store"), None, "tensor"),
        P(("groups", "store"), None, None, "tensor"),
        P(("groups", "store"), None),
        P(("groups", "store"), None),
        P(("groups", "store")),
    )
    out_specs = P(("groups", "store"), "tensor")
    return jax.shard_map(body, mesh=mesh, in_specs=in_specs, out_specs=out_specs, check_vma=False)
```

```python
import functools

import jax
import jax.numpy as jnp
from jax import lax
from jax.experimental import pallas as pl
from jax.experimental.pallas import tpu as pltpu
from jax.sharding import PartitionSpec as P

HEAD_DIM = 128
REACH = 4
MASKED = -1e30
FLOOR = -1e29
MESH = pl.DeviceIdType.MESH


def plan(places, owners, lengths, owner, seq_count, most_pages, capacity):
    pages = [jnp.int32(0)] * capacity
    seqs = [jnp.int32(-1)] * capacity
    rank = jnp.int32(0)
    for s in range(seq_count):
        length = lengths[0, s]
        for j in range(most_pages):
            hit = jnp.logical_and(j < length, owners[s, j] == owner)
            for c in range(capacity):
                mine = jnp.logical_and(hit, rank == c)
                pages[c] = jnp.where(mine, places[s, j], pages[c])
                seqs[c] = jnp.where(mine, s, seqs[c])
            rank = rank + hit.astype(jnp.int32)
    return pages + seqs


def kernel(
    n, seq_count, most_pages, capacity, kv_count, rows, order, scale,
    q_ref, fresh_ref, kv_ref, places_ref, owners_ref, lengths_ref, out_ref,
    key_shelf, value_shelf, q_in, fresh, places, owners, lengths, wants, asked, part_out, part_in,
    shelf_sem, local_sem, ask_send, ask_recv, back_send, back_recv,
):
    me = lax.axis_index("store")

    def at(steps):
        return {"store": lax.rem(me + steps + n, n)}

    loads = [
        pltpu.make_async_copy(kv_ref.at[:, i], half, shelf_sem.at[i])
        for i, half in enumerate((key_shelf, value_shelf))
    ]
    locals_ = [
        pltpu.make_async_copy(source, target, local_sem.at[i])
        for i, (source, target) in enumerate(
            (
                (places_ref, places),
                (owners_ref, owners),
                (lengths_ref, lengths),
                (q_ref, q_in.at[0]),
                (fresh_ref, fresh),
            )
        )
    ]

    barrier = pltpu.get_barrier_semaphore()
    for d in range(1, REACH):
        pl.semaphore_signal(barrier, inc=1, device_id=at(-d), device_id_type=MESH)
    for copy in locals_ + loads:
        copy.start()
    for copy in locals_:
        copy.wait()
    for d in range(REACH):
        owner = lax.rem(me + d, n)
        wanted = plan(places, owners, lengths, owner, seq_count, most_pages, capacity)
        for i, word in enumerate(wanted):
            wants[d, 0, i] = word
    pl.semaphore_wait(barrier, REACH - 1)

    asks = {}
    for d in order:
        asks[d] = [
            pltpu.make_async_remote_copy(
                src_ref=source,
                dst_ref=target.at[d],
                send_sem=ask_send.at[i, d - 1],
                recv_sem=ask_recv.at[i, d - 1],
                device_id=at(d),
                device_id_type=MESH,
            )
            for i, (source, target) in enumerate(((wants.at[d], asked), (q_in.at[0], q_in)))
        ]
        for copy in asks[d]:
            copy.start()

    turn = lax.rem(lax.broadcasted_iota(jnp.int32, (rows, 1), 0), seq_count)
    lane = lax.broadcasted_iota(jnp.int32, (rows, HEAD_DIM), 1)

    def partial_of(words, slot, wait_values=None):
        pages = [words[slot, 0, c] for c in range(capacity)]
        seqs = [words[slot, 0, capacity + c] for c in range(capacity)]
        bias = [jnp.where(turn == seq, jnp.float32(0.0), jnp.float32(MASKED)) for seq in seqs]
        scores = []
        for k in range(kv_count):
            qk = q_in[slot, k * rows : (k + 1) * rows, :]
            row = []
            for c in range(capacity):
                keys = key_shelf[pages[c], :, k * HEAD_DIM : (k + 1) * HEAD_DIM]
                dots = lax.dot_general(
                    qk, keys, (((1,), (1,)), ((), ())), preferred_element_type=jnp.float32
                )
                row.append(dots * scale + bias[c])
            scores.append(row)
        if wait_values is not None:
            wait_values()
        peaks, totals, sums = [], [], []
        for k in range(kv_count):
            peak = functools.reduce(jnp.maximum, [jnp.max(s, axis=1, keepdims=True) for s in scores[k]])
            peak = jnp.maximum(peak, jnp.float32(FLOOR))
            total = jnp.float32(0.0)
            summed = jnp.float32(0.0)
            for c in range(capacity):
                w = jnp.exp(scores[k][c] - peak)
                total = total + jnp.sum(w, axis=1, keepdims=True)
                high = w.astype(jnp.bfloat16)
                low = (w - high.astype(jnp.float32)).astype(jnp.bfloat16)
                values = value_shelf[pages[c], :, k * HEAD_DIM : (k + 1) * HEAD_DIM]
                summed = summed + jnp.dot(
                    jnp.concatenate([high, low], axis=0), values, preferred_element_type=jnp.float32
                )
            peaks.append(peak)
            totals.append(total)
            sums.append(summed[:rows] + summed[rows:])
        return peaks, totals, sums

    loads[0].wait()
    peaks, totals, sums = partial_of(wants, 0, loads[1].wait)
    for k in range(kv_count):
        qk = q_in[0, k * rows : (k + 1) * rows, :].astype(jnp.float32)
        cut = slice(k * HEAD_DIM, (k + 1) * HEAD_DIM)
        key = fresh[0, 0:1, cut].astype(jnp.float32)
        value = fresh[0, 1:2, cut].astype(jnp.float32)
        for s in range(1, seq_count):
            key = jnp.where(turn == s, fresh[s, 0:1, cut].astype(jnp.float32), key)
            value = jnp.where(turn == s, fresh[s, 1:2, cut].astype(jnp.float32), value)
        own = jnp.sum(qk * key, axis=1, keepdims=True) * scale
        peak = jnp.maximum(peaks[k], own)
        factor = jnp.exp(peaks[k] - peak)
        weight = jnp.exp(own - peak)
        peaks[k] = peak
        totals[k] = totals[k] * factor + weight
        sums[k] = sums[k] * factor + weight * value

    backs = {}
    for d in order:
        for copy in asks[d]:
            copy.wait_recv()
        theirs = partial_of(asked, d)
        stats = jnp.zeros((rows, HEAD_DIM), jnp.float32)
        for k in range(kv_count):
            part_out[d - 1, k * rows : (k + 1) * rows, :] = theirs[2][k]
            stats = jnp.where(lane == 2 * k, theirs[0][k], stats)
            stats = jnp.where(lane == 2 * k + 1, theirs[1][k], stats)
        part_out[d - 1, kv_count * rows :, :] = stats
        backs[d] = pltpu.make_async_remote_copy(
            src_ref=part_out.at[d - 1],
            dst_ref=part_in.at[d - 1],
            send_sem=back_send.at[d - 1],
            recv_sem=back_recv.at[d - 1],
            device_id=at(-d),
            device_id_type=MESH,
        )
        backs[d].start()

    for d in order:
        backs[d].wait_recv()
        for k in range(kv_count):
            part_peak = part_in[d - 1, kv_count * rows :, 2 * k : 2 * k + 1]
            part_total = part_in[d - 1, kv_count * rows :, 2 * k + 1 : 2 * k + 2]
            peak = jnp.maximum(peaks[k], part_peak)
            factor = jnp.exp(peaks[k] - peak)
            part_factor = jnp.exp(part_peak - peak)
            peaks[k] = peak
            totals[k] = totals[k] * factor + part_total * part_factor
            sums[k] = sums[k] * factor + part_in[d - 1, k * rows : (k + 1) * rows, :] * part_factor
    for k in range(kv_count):
        out_ref[k * rows : (k + 1) * rows, :] = (sums[k] / totals[k]).astype(out_ref.dtype)
    for d in order:
        for copy in asks[d]:
            copy.wait_send()
        backs[d].wait_send()


def body(queries, new_kv, kv_pages, page_index, page_owner, seq_pages):
    n = lax.axis_size("store")
    seq_count, most_pages = page_index.shape
    kv_count = new_kv.shape[2] // HEAD_DIM
    heads = queries.shape[1] // HEAD_DIM
    rows = heads // kv_count * seq_count
    all_rows = heads * seq_count
    capacity = seq_count * most_pages // REACH
    q = queries.reshape(seq_count, heads, HEAD_DIM).transpose(1, 0, 2).reshape(all_rows, HEAD_DIM)
    away = REACH - 1
    half = kv_pages.shape[:1] + kv_pages.shape[2:]
    order = (1, 2, 3)
    out = pl.pallas_call(
        functools.partial(
            kernel, n, seq_count, most_pages, capacity, kv_count, rows, order, HEAD_DIM ** (-0.5)
        ),
        out_shape=pltpu.VMEM((all_rows, HEAD_DIM), jnp.bfloat16),
        in_specs=[pl.BlockSpec(memory_space=pl.ANY)] * 6,
        out_specs=pl.BlockSpec(memory_space=pltpu.VMEM),
        scratch_shapes=[
            pltpu.VMEM(half, kv_pages.dtype),
            pltpu.VMEM(half, kv_pages.dtype),
            pltpu.VMEM((REACH, all_rows, HEAD_DIM), q.dtype),
            pltpu.VMEM(new_kv.shape, new_kv.dtype),
            pltpu.SMEM(page_index.shape, jnp.int32),
            pltpu.SMEM(page_owner.shape, jnp.int32),
            pltpu.SMEM((1, seq_count), jnp.int32),
            pltpu.SMEM((REACH, 1, 2 * capacity), jnp.int32),
            pltpu.SMEM((REACH, 1, 2 * capacity), jnp.int32),
            pltpu.VMEM((away, all_rows + rows, HEAD_DIM), jnp.float32),
            pltpu.VMEM((away, all_rows + rows, HEAD_DIM), jnp.float32),
            pltpu.SemaphoreType.DMA((2,)),
            pltpu.SemaphoreType.DMA((5,)),
            pltpu.SemaphoreType.DMA((2, away)),
            pltpu.SemaphoreType.DMA((2, away)),
            pltpu.SemaphoreType.DMA((away,)),
            pltpu.SemaphoreType.DMA((away,)),
        ],
        compiler_params=pltpu.CompilerParams(collective_id=0, has_side_effects=True),
    )(q, new_kv, kv_pages, page_index, page_owner, seq_pages.reshape(1, seq_count))
    out = out.reshape(heads, seq_count, HEAD_DIM).transpose(1, 0, 2)
    return out.reshape(seq_count, heads * HEAD_DIM)


def solution(mesh):
    in_specs = (
        P(("groups", "store"), "tensor"),
        P(("groups", "store"), None, "tensor"),
        P(("groups", "store"), None, None, "tensor"),
        P(("groups", "store"), None),
        P(("groups", "store"), None),
        P(("groups", "store")),
    )
    out_specs = P(("groups", "store"), "tensor")
    return jax.shard_map(body, mesh=mesh, in_specs=in_specs, out_specs=out_specs, check_vma=False)
```

```python
import functools

import jax
import jax.numpy as jnp
from jax import lax
from jax.experimental import pallas as pl
from jax.experimental.pallas import tpu as pltpu
from jax.sharding import PartitionSpec as P

HEAD_DIM = 128
REACH = 4
MASKED = -1e30
FLOOR = -1e29
MESH = pl.DeviceIdType.MESH


def plan(places, owners, lengths, owner, seq_count, most_pages, capacity):
    pages = [jnp.int32(0)] * capacity
    seqs = [jnp.int32(-1)] * capacity
    rank = jnp.int32(0)
    for s in range(seq_count):
        length = lengths[0, s]
        for j in range(most_pages):
            hit = jnp.logical_and(j < length, owners[s, j] == owner)
            for c in range(capacity):
                mine = jnp.logical_and(hit, rank == c)
                pages[c] = jnp.where(mine, places[s, j], pages[c])
                seqs[c] = jnp.where(mine, s, seqs[c])
            rank = rank + hit.astype(jnp.int32)
    return pages + seqs


def kernel(
    n, seq_count, most_pages, capacity, kv_count, rows, order, scale,
    q_ref, fresh_ref, kv_ref, places_ref, owners_ref, lengths_ref, out_ref,
    key_shelf, value_shelf, turned, q_in, fresh, places, owners, lengths, wants, asked, part_out, part_in,
    shelf_sem, local_sem, ask_send, ask_recv, back_send, back_recv,
):
    me = lax.axis_index("store")

    def at(steps):
        return {"store": lax.rem(me + steps + n, n)}

    loads = [
        pltpu.make_async_copy(kv_ref.at[:, i], half, shelf_sem.at[i])
        for i, half in enumerate((key_shelf, value_shelf))
    ]
    locals_ = [
        pltpu.make_async_copy(source, target, local_sem.at[i])
        for i, (source, target) in enumerate(
            (
                (places_ref, places),
                (owners_ref, owners),
                (lengths_ref, lengths),
                (q_ref, q_in.at[0]),
                (fresh_ref, fresh),
            )
        )
    ]

    barrier = pltpu.get_barrier_semaphore()
    for d in range(1, REACH):
        pl.semaphore_signal(barrier, inc=1, device_id=at(-d), device_id_type=MESH)
    for copy in locals_ + loads:
        copy.start()
    for copy in locals_:
        copy.wait()
    for d in range(REACH):
        owner = lax.rem(me + d, n)
        wanted = plan(places, owners, lengths, owner, seq_count, most_pages, capacity)
        for i, word in enumerate(wanted):
            wants[d, 0, i] = word
    pl.semaphore_wait(barrier, REACH - 1)

    asks = {}
    for d in order:
        asks[d] = [
            pltpu.make_async_remote_copy(
                src_ref=source,
                dst_ref=target.at[d],
                send_sem=ask_send.at[i, d - 1],
                recv_sem=ask_recv.at[i, d - 1],
                device_id=at(d),
                device_id_type=MESH,
            )
            for i, (source, target) in enumerate(((wants.at[d], asked), (q_in.at[0], q_in)))
        ]
        for copy in asks[d]:
            copy.start()

    turn = lax.rem(lax.broadcasted_iota(jnp.int32, (rows, 1), 0), seq_count)
    lane = lax.broadcasted_iota(jnp.int32, (rows, HEAD_DIM), 1)

    def partial_of(words, slot, wait_values=None):
        pages = [words[slot, 0, c] for c in range(capacity)]
        seqs = [words[slot, 0, capacity + c] for c in range(capacity)]
        bias = [jnp.where(turn == seq, jnp.float32(0.0), jnp.float32(MASKED)) for seq in seqs]
        scores = []
        for k in range(kv_count):
            qk = q_in[slot, k * rows : (k + 1) * rows, :]
            row = []
            for c in range(capacity):
                cut = slice(k * HEAD_DIM, (k + 1) * HEAD_DIM)
                keys, inner = (key_shelf[pages[c], :, cut], 1) if slot == 0 else (turned[pages[c], cut, :], 0)
                dots = lax.dot_general(
                    qk, keys, (((1,), (inner,)), ((), ())), preferred_element_type=jnp.float32
                )
                row.append(dots * scale + bias[c])
            scores.append(row)
        if wait_values is not None:
            wait_values()
        peaks, totals, sums = [], [], []
        for k in range(kv_count):
            peak = functools.reduce(jnp.maximum, [jnp.max(s, axis=1, keepdims=True) for s in scores[k]])
            peak = jnp.maximum(peak, jnp.float32(FLOOR))
            total = jnp.float32(0.0)
            summed = jnp.float32(0.0)
            for c in range(capacity):
                w = jnp.exp(scores[k][c] - peak)
                total = total + jnp.sum(w, axis=1, keepdims=True)
                high = w.astype(jnp.bfloat16)
                low = (w - high.astype(jnp.float32)).astype(jnp.bfloat16)
                values = value_shelf[pages[c], :, k * HEAD_DIM : (k + 1) * HEAD_DIM]
                summed = summed + jnp.dot(
                    jnp.concatenate([high, low], axis=0), values, preferred_element_type=jnp.float32
                )
            peaks.append(peak)
            totals.append(total)
            sums.append(summed[:rows] + summed[rows:])
        return peaks, totals, sums

    loads[0].wait()
    peaks, totals, sums = partial_of(wants, 0, loads[1].wait)
    for k in range(kv_count):
        qk = q_in[0, k * rows : (k + 1) * rows, :].astype(jnp.float32)
        cut = slice(k * HEAD_DIM, (k + 1) * HEAD_DIM)
        key = fresh[0, 0:1, cut].astype(jnp.float32)
        value = fresh[0, 1:2, cut].astype(jnp.float32)
        for s in range(1, seq_count):
            key = jnp.where(turn == s, fresh[s, 0:1, cut].astype(jnp.float32), key)
            value = jnp.where(turn == s, fresh[s, 1:2, cut].astype(jnp.float32), value)
        own = jnp.sum(qk * key, axis=1, keepdims=True) * scale
        peak = jnp.maximum(peaks[k], own)
        factor = jnp.exp(peaks[k] - peak)
        weight = jnp.exp(own - peak)
        peaks[k] = peak
        totals[k] = totals[k] * factor + weight
        sums[k] = sums[k] * factor + weight * value

    @pl.loop(0, key_shelf.shape[0])
    def _(page):
        for k in range(kv_count):
            cut = slice(k * HEAD_DIM, (k + 1) * HEAD_DIM)
            turned[page, cut, :] = key_shelf[page, :, cut].T

    backs = {}
    for d in order:
        for copy in asks[d]:
            copy.wait_recv()
        theirs = partial_of(asked, d)
        stats = jnp.zeros((rows, HEAD_DIM), jnp.float32)
        for k in range(kv_count):
            part_out[d - 1, k * rows : (k + 1) * rows, :] = theirs[2][k]
            stats = jnp.where(lane == 2 * k, theirs[0][k], stats)
            stats = jnp.where(lane == 2 * k + 1, theirs[1][k], stats)
        part_out[d - 1, kv_count * rows :, :] = stats
        backs[d] = pltpu.make_async_remote_copy(
            src_ref=part_out.at[d - 1],
            dst_ref=part_in.at[d - 1],
            send_sem=back_send.at[d - 1],
            recv_sem=back_recv.at[d - 1],
            device_id=at(-d),
            device_id_type=MESH,
        )
        backs[d].start()

    for d in order:
        backs[d].wait_recv()
        for k in range(kv_count):
            part_peak = part_in[d - 1, kv_count * rows :, 2 * k : 2 * k + 1]
            part_total = part_in[d - 1, kv_count * rows :, 2 * k + 1 : 2 * k + 2]
            peak = jnp.maximum(peaks[k], part_peak)
            factor = jnp.exp(peaks[k] - peak)
            part_factor = jnp.exp(part_peak - peak)
            peaks[k] = peak
            totals[k] = totals[k] * factor + part_total * part_factor
            sums[k] = sums[k] * factor + part_in[d - 1, k * rows : (k + 1) * rows, :] * part_factor
    for k in range(kv_count):
        out_ref[k * rows : (k + 1) * rows, :] = (sums[k] / totals[k]).astype(out_ref.dtype)
    for d in order:
        for copy in asks[d]:
            copy.wait_send()
        backs[d].wait_send()


def body(queries, new_kv, kv_pages, page_index, page_owner, seq_pages):
    n = lax.axis_size("store")
    seq_count, most_pages = page_index.shape
    kv_count = new_kv.shape[2] // HEAD_DIM
    heads = queries.shape[1] // HEAD_DIM
    rows = heads // kv_count * seq_count
    all_rows = heads * seq_count
    capacity = seq_count * most_pages // REACH
    q = queries.reshape(seq_count, heads, HEAD_DIM).transpose(1, 0, 2).reshape(all_rows, HEAD_DIM)
    away = REACH - 1
    half = kv_pages.shape[:1] + kv_pages.shape[2:]
    order = (1, 2, 3)
    out = pl.pallas_call(
        functools.partial(
            kernel, n, seq_count, most_pages, capacity, kv_count, rows, order, HEAD_DIM ** (-0.5)
        ),
        out_shape=pltpu.VMEM((all_rows, HEAD_DIM), jnp.bfloat16),
        in_specs=[pl.BlockSpec(memory_space=pl.ANY)] * 6,
        out_specs=pl.BlockSpec(memory_space=pltpu.VMEM),
        scratch_shapes=[
            pltpu.VMEM(half, kv_pages.dtype),
            pltpu.VMEM(half, kv_pages.dtype),
            pltpu.VMEM((half[0], half[2], half[1]), kv_pages.dtype),
            pltpu.VMEM((REACH, all_rows, HEAD_DIM), q.dtype),
            pltpu.VMEM(new_kv.shape, new_kv.dtype),
            pltpu.SMEM(page_index.shape, jnp.int32),
            pltpu.SMEM(page_owner.shape, jnp.int32),
            pltpu.SMEM((1, seq_count), jnp.int32),
            pltpu.SMEM((REACH, 1, 2 * capacity), jnp.int32),
            pltpu.SMEM((REACH, 1, 2 * capacity), jnp.int32),
            pltpu.VMEM((away, all_rows + rows, HEAD_DIM), jnp.float32),
            pltpu.VMEM((away, all_rows + rows, HEAD_DIM), jnp.float32),
            pltpu.SemaphoreType.DMA((2,)),
            pltpu.SemaphoreType.DMA((5,)),
            pltpu.SemaphoreType.DMA((2, away)),
            pltpu.SemaphoreType.DMA((2, away)),
            pltpu.SemaphoreType.DMA((away,)),
            pltpu.SemaphoreType.DMA((away,)),
        ],
        compiler_params=pltpu.CompilerParams(collective_id=0, has_side_effects=True),
    )(q, new_kv, kv_pages, page_index, page_owner, seq_pages.reshape(1, seq_count))
    out = out.reshape(heads, seq_count, HEAD_DIM).transpose(1, 0, 2)
    return out.reshape(seq_count, heads * HEAD_DIM)


def solution(mesh):
    in_specs = (
        P(("groups", "store"), "tensor"),
        P(("groups", "store"), None, "tensor"),
        P(("groups", "store"), None, None, "tensor"),
        P(("groups", "store"), None),
        P(("groups", "store"), None),
        P(("groups", "store")),
    )
    out_specs = P(("groups", "store"), "tensor")
    return jax.shard_map(body, mesh=mesh, in_specs=in_specs, out_specs=out_specs, check_vma=False)
```

```python
import functools

import jax
import jax.numpy as jnp
from jax import lax
from jax.experimental import pallas as pl
from jax.experimental.pallas import tpu as pltpu
from jax.sharding import PartitionSpec as P

HEAD_DIM = 128
REACH = 4
MASKED = -1e30
FLOOR = -1e29
MESH = pl.DeviceIdType.MESH


def plan(places, owners, lengths, owner, seq_count, most_pages, capacity):
    pages = [jnp.int32(0)] * capacity
    seqs = [jnp.int32(-1)] * capacity
    rank = jnp.int32(0)
    for s in range(seq_count):
        length = lengths[0, s]
        for j in range(most_pages):
            hit = jnp.logical_and(j < length, owners[s, j] == owner)
            for c in range(capacity):
                mine = jnp.logical_and(hit, rank == c)
                pages[c] = jnp.where(mine, places[s, j], pages[c])
                seqs[c] = jnp.where(mine, s, seqs[c])
            rank = rank + hit.astype(jnp.int32)
    return pages + seqs


def kernel(
    n, seq_count, most_pages, capacity, kv_count, rows, order, scale,
    q_ref, fresh_ref, kv_ref, places_ref, owners_ref, lengths_ref, out_ref,
    key_shelf, value_shelf, turned, q_in, fresh, places, owners, lengths, wants, asked, part_out, part_in,
    shelf_sem, local_sem, ask_send, ask_recv, back_send, back_recv,
):
    me = lax.axis_index("store")

    def at(steps):
        return {"store": lax.rem(me + steps + n, n)}

    loads = [
        pltpu.make_async_copy(kv_ref.at[:, i], half, shelf_sem.at[i])
        for i, half in enumerate((key_shelf, value_shelf))
    ]
    locals_ = [
        pltpu.make_async_copy(source, target, local_sem.at[i])
        for i, (source, target) in enumerate(
            (
                (places_ref, places),
                (owners_ref, owners),
                (lengths_ref, lengths),
                (q_ref, q_in.at[0]),
                (fresh_ref, fresh),
            )
        )
    ]

    barrier = pltpu.get_barrier_semaphore()
    for d in range(1, REACH):
        pl.semaphore_signal(barrier, inc=1, device_id=at(-d), device_id_type=MESH)
    for copy in locals_ + loads:
        copy.start()
    for copy in locals_:
        copy.wait()
    for d in range(REACH):
        owner = lax.rem(me + d, n)
        wanted = plan(places, owners, lengths, owner, seq_count, most_pages, capacity)
        for i, word in enumerate(wanted):
            wants[d, 0, i] = word
    pl.semaphore_wait(barrier, REACH - 1)

    asks = {}
    for d in order:
        asks[d] = [
            pltpu.make_async_remote_copy(
                src_ref=source,
                dst_ref=target.at[d],
                send_sem=ask_send.at[i, d - 1],
                recv_sem=ask_recv.at[i, d - 1],
                device_id=at(d),
                device_id_type=MESH,
            )
            for i, (source, target) in enumerate(((wants.at[d], asked), (q_in.at[0], q_in)))
        ]
        for copy in asks[d]:
            copy.start()

    turn = lax.rem(lax.broadcasted_iota(jnp.int32, (rows, 1), 0), seq_count)
    lane = lax.broadcasted_iota(jnp.int32, (rows, HEAD_DIM), 1)

    def partial_of(words, slot, wait_values=None):
        pages = [words[slot, 0, c] for c in range(capacity)]
        seqs = [words[slot, 0, capacity + c] for c in range(capacity)]
        bias = [jnp.where(turn == seq, jnp.float32(0.0), jnp.float32(MASKED)) for seq in seqs]
        scores = []
        for k in range(kv_count):
            qk = q_in[slot, k * rows : (k + 1) * rows, :]
            row = []
            for c in range(capacity):
                cut = slice(k * HEAD_DIM, (k + 1) * HEAD_DIM)
                keys, inner = (key_shelf[pages[c], :, cut], 1) if slot == 0 else (turned[pages[c], cut, :], 0)
                dots = lax.dot_general(
                    qk, keys, (((1,), (inner,)), ((), ())), preferred_element_type=jnp.float32
                )
                row.append(dots * scale + bias[c])
            scores.append(row)
        if wait_values is not None:
            wait_values()
        peaks, totals, sums = [], [], []
        for k in range(kv_count):
            peak = functools.reduce(jnp.maximum, [jnp.max(s, axis=1, keepdims=True) for s in scores[k]])
            peak = jnp.maximum(peak, jnp.float32(FLOOR))
            total = jnp.float32(0.0)
            summed = jnp.float32(0.0)
            for c in range(capacity):
                w = jnp.exp(scores[k][c] - peak)
                total = total + jnp.sum(w, axis=1, keepdims=True)
                high = w.astype(jnp.bfloat16)
                low = (w - high.astype(jnp.float32)).astype(jnp.bfloat16)
                values = value_shelf[pages[c], :, k * HEAD_DIM : (k + 1) * HEAD_DIM]
                summed = summed + jnp.dot(
                    jnp.concatenate([high, low], axis=0), values, preferred_element_type=jnp.float32
                )
            peaks.append(peak)
            totals.append(total)
            sums.append(summed[:rows] + summed[rows:])
        return peaks, totals, sums

    loads[0].wait()
    peaks, totals, sums = partial_of(wants, 0, loads[1].wait)
    for k in range(kv_count):
        qk = q_in[0, k * rows : (k + 1) * rows, :].astype(jnp.float32)
        cut = slice(k * HEAD_DIM, (k + 1) * HEAD_DIM)
        key = fresh[0, 0:1, cut].astype(jnp.float32)
        value = fresh[0, 1:2, cut].astype(jnp.float32)
        for s in range(1, seq_count):
            key = jnp.where(turn == s, fresh[s, 0:1, cut].astype(jnp.float32), key)
            value = jnp.where(turn == s, fresh[s, 1:2, cut].astype(jnp.float32), value)
        own = jnp.sum(qk * key, axis=1, keepdims=True) * scale
        peak = jnp.maximum(peaks[k], own)
        factor = jnp.exp(peaks[k] - peak)
        weight = jnp.exp(own - peak)
        peaks[k] = peak
        totals[k] = totals[k] * factor + weight
        sums[k] = sums[k] * factor + weight * value

    @pl.loop(0, key_shelf.shape[0])
    def _(page):
        for k in range(kv_count):
            cut = slice(k * HEAD_DIM, (k + 1) * HEAD_DIM)
            turned[page, cut, :] = key_shelf[page, :, cut].T

    backs = {}
    for d in order:
        for copy in asks[d]:
            copy.wait_recv()
        theirs = partial_of(asked, d)
        stats = jnp.zeros((rows, HEAD_DIM), jnp.float32)
        for k in range(kv_count):
            stats = jnp.where(lane == 2 * k, theirs[0][k], stats)
            stats = jnp.where(lane == 2 * k + 1, theirs[1][k], stats)
        part_out[d - 1, :rows, :] = stats
        cuts = (0, (1 + kv_count // 2) * rows, (1 + kv_count) * rows)
        backs[d] = []
        for i in range(2):
            for k in range(kv_count):
                at_row = (1 + k) * rows
                if cuts[i] <= at_row < cuts[i + 1]:
                    part_out[d - 1, at_row : at_row + rows, :] = theirs[2][k]
            window = pl.ds(cuts[i], cuts[i + 1] - cuts[i])
            copy = pltpu.make_async_remote_copy(
                src_ref=part_out.at[d - 1, window],
                dst_ref=part_in.at[d - 1, window],
                send_sem=back_send.at[i, d - 1],
                recv_sem=back_recv.at[i, d - 1],
                device_id=at(-d),
                device_id_type=MESH,
            )
            copy.start()
            backs[d].append(copy)

    for d in order:
        for copy in backs[d]:
            copy.wait_recv()
        for k in range(kv_count):
            part_peak = part_in[d - 1, :rows, 2 * k : 2 * k + 1]
            part_total = part_in[d - 1, :rows, 2 * k + 1 : 2 * k + 2]
            peak = jnp.maximum(peaks[k], part_peak)
            factor = jnp.exp(peaks[k] - peak)
            part_factor = jnp.exp(part_peak - peak)
            peaks[k] = peak
            totals[k] = totals[k] * factor + part_total * part_factor
            sums[k] = sums[k] * factor + part_in[d - 1, (k + 1) * rows : (k + 2) * rows, :] * part_factor
    for k in range(kv_count):
        out_ref[k * rows : (k + 1) * rows, :] = (sums[k] / totals[k]).astype(out_ref.dtype)
    for d in order:
        for copy in asks[d]:
            copy.wait_send()
        for copy in backs[d]:
            copy.wait_send()


def body(queries, new_kv, kv_pages, page_index, page_owner, seq_pages):
    n = lax.axis_size("store")
    seq_count, most_pages = page_index.shape
    kv_count = new_kv.shape[2] // HEAD_DIM
    heads = queries.shape[1] // HEAD_DIM
    rows = heads // kv_count * seq_count
    all_rows = heads * seq_count
    capacity = seq_count * most_pages // REACH
    q = queries.reshape(seq_count, heads, HEAD_DIM).transpose(1, 0, 2).reshape(all_rows, HEAD_DIM)
    away = REACH - 1
    half = kv_pages.shape[:1] + kv_pages.shape[2:]
    order = (1, 2, 3)
    out = pl.pallas_call(
        functools.partial(
            kernel, n, seq_count, most_pages, capacity, kv_count, rows, order, HEAD_DIM ** (-0.5)
        ),
        out_shape=pltpu.VMEM((all_rows, HEAD_DIM), jnp.bfloat16),
        in_specs=[pl.BlockSpec(memory_space=pl.ANY)] * 6,
        out_specs=pl.BlockSpec(memory_space=pltpu.VMEM),
        scratch_shapes=[
            pltpu.VMEM(half, kv_pages.dtype),
            pltpu.VMEM(half, kv_pages.dtype),
            pltpu.VMEM((half[0], half[2], half[1]), kv_pages.dtype),
            pltpu.VMEM((REACH, all_rows, HEAD_DIM), q.dtype),
            pltpu.VMEM(new_kv.shape, new_kv.dtype),
            pltpu.SMEM(page_index.shape, jnp.int32),
            pltpu.SMEM(page_owner.shape, jnp.int32),
            pltpu.SMEM((1, seq_count), jnp.int32),
            pltpu.SMEM((REACH, 1, 2 * capacity), jnp.int32),
            pltpu.SMEM((REACH, 1, 2 * capacity), jnp.int32),
            pltpu.VMEM((away, all_rows + rows, HEAD_DIM), jnp.float32),
            pltpu.VMEM((away, all_rows + rows, HEAD_DIM), jnp.float32),
            pltpu.SemaphoreType.DMA((2,)),
            pltpu.SemaphoreType.DMA((5,)),
            pltpu.SemaphoreType.DMA((2, away)),
            pltpu.SemaphoreType.DMA((2, away)),
            pltpu.SemaphoreType.DMA((2, away)),
            pltpu.SemaphoreType.DMA((2, away)),
        ],
        compiler_params=pltpu.CompilerParams(collective_id=0, has_side_effects=True),
    )(q, new_kv, kv_pages, page_index, page_owner, seq_pages.reshape(1, seq_count))
    out = out.reshape(heads, seq_count, HEAD_DIM).transpose(1, 0, 2)
    return out.reshape(seq_count, heads * HEAD_DIM)


def solution(mesh):
    in_specs = (
        P(("groups", "store"), "tensor"),
        P(("groups", "store"), None, "tensor"),
        P(("groups", "store"), None, None, "tensor"),
        P(("groups", "store"), None),
        P(("groups", "store"), None),
        P(("groups", "store")),
    )
    out_specs = P(("groups", "store"), "tensor")
    return jax.shard_map(body, mesh=mesh, in_specs=in_specs, out_specs=out_specs, check_vma=False)
```
